64 devices in a mesh: rep: 8 (over x, y, core), dp: 8 (over z).
Axes of the slice: x: 2, y: 2, z: 8, core: 2. Of those that a mesh axis runs over, the one named last changes fastest.
The devices are a block of a 4x4x8 slice.
Arguments:
- x: bfloat16 [64, 4096, 512], P(('rep', 'dp')), parts along dimension 0
- dy: bfloat16 [64, 4096, 512], P(('rep', 'dp')), parts along dimension 0
- w_gate: bfloat16 [2, 512, 2048], replicated
- w_up: bfloat16 [2, 512, 2048], replicated
- w_down: bfloat16 [2, 2048, 512], replicated
- m_w_gate: float32 [2, 512, 2048], P(None, 'dp')
- m_w_up: float32 [2, 512, 2048], P(None, 'dp')
- m_w_down: float32 [2, 2048, 512], P(None, 'dp')
- v_w_gate: float32 [2, 512, 2048], P(None, 'dp')
- v_w_up: float32 [2, 512, 2048], P(None, 'dp')
- v_w_down: float32 [2, 2048, 512], P(None, 'dp')
Outputs:
- output 1: bfloat16 [16, 512, 2048], P('rep'), parts along dimension 0
- output 2: bfloat16 [16, 512, 2048], P('rep'), parts along dimension 0
- output 3: bfloat16 [16, 2048, 512], P('rep'), parts along dimension 0
- output 4: float32 [16, 512, 2048], P('rep', 'dp'), parts along dimension 0
- output 5: float32 [16, 512, 2048], P('rep', 'dp'), parts along dimension 0
- output 6: float32 [16, 2048, 512], P('rep', 'dp'), parts along dimension 0
- output 7: float32 [16, 512, 2048], P('rep', 'dp'), parts along dimension 0
- output 8: float32 [16, 512, 2048], P('rep', 'dp'), parts along dimension 0
- output 9: float32 [16, 2048, 512], P('rep', 'dp'), parts along dimension 0
There are 8 independent parts. The reference program is written for one: setup_inputs(seed, part) draws one part's arguments, and reference() takes and returns one part's arrays. A program takes and returns all parts, laid end to end along the dimension named above; an argument that names none is the same for every part.
All inputs are finite; a program needn't handle non-finite values.
Results may differ from the reference program's by a relative error of at most 0.02.
Values are sent between devices in bfloat16 or wider.
A program may use at most 768 MiB of HBM per device.

```python
import jax
import jax.numpy as jnp
from jax import lax

SEQUENCES = 8
TOKENS = 4096
D = 512
FF = 2048
LAYERS = 2
NAMES = ("w_gate", "w_up", "w_down")
SHAPES = {"w_gate": (LAYERS, D, FF), "w_up": (LAYERS, D, FF), "w_down": (LAYERS, FF, D)}


def bump(key, n, height):
    away = (jnp.arange(n, dtype=jnp.int32) - jax.random.randint(key, (), 0, n, jnp.int32)) % n
    return jnp.where(away < n // 8, height, 1.0)


def together(key, own, strength):
    shared = jax.random.normal(key, own.shape[1:], jnp.float32)
    return (own + strength * shared) * lax.rsqrt(1 + strength * strength)


def setup_inputs(seed: int = 0, part: int = 0) -> dict:
    kx, kdy, ka, kb, kz, kf, kh, kl, *keys = jax.random.split(jax.random.key(seed), 8 + 3 * len(NAMES))
    kx, kdy, ka, kb = (jax.random.fold_in(k, part) for k in (kx, kdy, ka, kb))
    kw, km, kv = (keys[i::3] for i in range(3))
    shape = (SEQUENCES, TOKENS, D)
    much_x, much_dy = jax.random.uniform(kz, (2,), jnp.float32, 0.0, 1.0)
    loud = 2.0 ** jax.random.uniform(jax.random.fold_in(kz, 1), (), jnp.float32, -1.0, 2.0)
    layers = 2.0 ** jax.random.uniform(kl, (LAYERS, 1, 1), jnp.float32, -1.0, 1.0)
    x = together(ka, jax.random.normal(kx, shape, jnp.float32), much_x) * bump(kf, D, 4.0)
    dy = together(kb, jax.random.normal(kdy, shape, jnp.float32), much_dy)
    drawn = {"x": x.astype(jnp.bfloat16), "dy": (loud * dy * (SEQUENCES * TOKENS) ** -0.5).astype(jnp.bfloat16)}
    for key, name in zip(kw, NAMES, strict=True):
        w = jax.random.normal(key, SHAPES[name], jnp.float32) * SHAPES[name][1] ** -0.5
        drawn[name] = (w * {"w_gate": 1.0, "w_up": bump(kh, FF, 4.0), "w_down": layers}[name]).astype(jnp.bfloat16)
    for key, name in zip(km, NAMES, strict=True):
        drawn[f"m_{name}"] = 0.1 * jax.random.normal(key, SHAPES[name], jnp.float32)
    for key, name in zip(kv, NAMES, strict=True):
        drawn[f"v_{name}"] = jax.random.uniform(key, SHAPES[name], jnp.float32, 0.005, 0.015)
    return drawn


def matmul(a, w):
    return jnp.dot(a, w, preferred_element_type=jnp.float32).astype(jnp.bfloat16)


def normed(h):
    wide = h.astype(jnp.float32)
    scale = lax.rsqrt(jnp.mean(wide**2, -1, keepdims=True) + 1e-6)
    return (wide * scale).astype(jnp.bfloat16)


def layer(h, w):
    a = normed(h)
    gate = jnp.dot(a, w["w_gate"], preferred_element_type=jnp.float32)
    up = jnp.dot(a, w["w_up"], preferred_element_type=jnp.float32)
    return h + matmul((jax.nn.silu(gate) * up).astype(jnp.bfloat16), w["w_down"])


def adamw(w, m, v, g):
    m = 0.9 * m + 0.1 * g
    v = 0.95 * v + 0.05 * g * g
    step = m * lax.rsqrt(v + 1e-8) + 0.1 * w
    return (w - 0.02 * step).astype(jnp.bfloat16), m, v


def stack(weights, h):
    return lax.scan(lambda h, w: (layer(h, w), None), h, weights)[0]


def reference(x, dy, w_gate, w_up, w_down, m_w_gate, m_w_up, m_w_down, v_w_gate, v_w_up, v_w_down):
    weights = dict(zip(NAMES, (w_gate, w_up, w_down), strict=True))

    def take(so_far, sequence):
        h, by_y = sequence
        _, back = jax.vjp(lambda w: stack(w, h), weights)
        return jax.tree.map(lambda total, term: total + term.astype(jnp.float32), so_far, back(by_y)[0]), None

    none_yet = {name: jnp.zeros(w.shape, jnp.float32) for name, w in weights.items()}
    by_weights, _ = lax.scan(take, none_yet, (x, dy))
    gradients = [by_weights[name].astype(jnp.bfloat16).astype(jnp.float32) for name in NAMES]
    new = [
        adamw(w.astype(jnp.float32), m, v, g)
        for w, m, v, g in zip((w_gate, w_up, w_down), (m_w_gate, m_w_up, m_w_down), (v_w_gate, v_w_up, v_w_down), gradients, strict=True)
    ]
    return tuple(one[which] for which in range(3) for one in new)
```

```python
import functools

import jax
import jax.numpy as jnp
from jax import lax
from jax.experimental import pallas as pl
from jax.experimental.pallas import tpu as pltpu
from jax.sharding import PartitionSpec as P

F32, BF = jnp.float32, jnp.bfloat16
NT = (((1,), (1,)), ((), ()))
MESH = pl.DeviceIdType.MESH
VMEM_LIMIT = 66_000_000
WIDE = 512
NARROW = 256
TILE = 512
ANY = pl.BlockSpec(memory_space=pl.ANY)
VMEM = pl.BlockSpec(memory_space=pltpu.VMEM)


def dot(a, b):
    return jnp.dot(a, b, preferred_element_type=F32)


def dot_nt(a, b):
    return lax.dot_general(a, b, NT, preferred_element_type=F32)


def sigmoid(g):
    return 0.5 * jnp.tanh(0.5 * g) + 0.5


def norm_scale(wide):
    return lax.rsqrt(jnp.mean(wide * wide, -1, keepdims=True) + 1e-6)


def adamw(w, m, v, g):
    m = 0.9 * m + 0.1 * g
    v = 0.95 * v + 0.05 * g * g
    step = m * lax.rsqrt(v + 1e-8) + 0.1 * w
    return (w - 0.02 * step).astype(BF), m, v


def forward_kernel(x_ref, dy_ref, wg_ref, wu_ref, wd_ref, h_ref, a0_ref, a1_ref, a0t_ref, a1t_ref, dyt_ref):
    x = x_ref[...].astype(F32)
    a = (x * norm_scale(x)).astype(BF)
    a0_ref[...] = a
    a0t_ref[...] = a.T
    dyt_ref[...] = dy_ref[...].T
    acc = None
    for at in range(0, wg_ref.shape[1], WIDE):
        cols = slice(at, at + WIDE)
        g = dot(a, wg_ref[:, cols])
        u = dot(a, wu_ref[:, cols])
        part = dot((g * sigmoid(g) * u).astype(BF), wd_ref[cols, :])
        acc = part if acc is None else acc + part
    h = (x + acc.astype(BF).astype(F32)).astype(BF)
    h_ref[...] = h
    wide = h.astype(F32)
    a1 = (wide * norm_scale(wide)).astype(BF)
    a1_ref[...] = a1
    a1t_ref[...] = a1.T


def forward(x, dy, wg, wu, wd):
    tokens, dim = x.shape
    row = pl.BlockSpec((TILE, dim), lambda i: (i, 0))
    col = pl.BlockSpec((dim, TILE), lambda i: (0, i))
    first = lambda w: pl.BlockSpec((None, *w.shape[1:]), lambda i: (0, 0, 0))
    return pl.pallas_call(
        forward_kernel,
        grid=(tokens // TILE,),
        in_specs=[row, row, first(wg), first(wu), first(wd)],
        out_specs=[row] * 3 + [col] * 3,
        out_shape=[jax.ShapeDtypeStruct((tokens, dim), BF)] * 3 + [jax.ShapeDtypeStruct((dim, tokens), BF)] * 3,
        compiler_params=pltpu.CompilerParams(vmem_limit_bytes=VMEM_LIMIT),
        name="forward0",
    )(x, dy, wg, wu, wd)


def rest_kernel(
    n, h_hbm, a0_hbm, a1_hbm, a0t_hbm, a1t_hbm, dyt_hbm, dy_hbm, wg_hbm, wu_hbm, wd_hbm, mg_hbm, mu_hbm, md_hbm, vg_hbm, vu_hbm, vd_hbm,
    og_ref, ou_ref, od_ref, gg_out, gu_out, gd_out,
    a_ref, at_ref, d_ref, dt_ref, da_ref, act_ref, dg_ref, du_ref, sg_ref, su_ref, sd_ref, tg_ref, tu_ref, td_ref,
    rg_ref, ru_ref, rc_ref, rw_ref, mg_ref, mu_ref, md_ref, vg_ref, vu_ref, vd_ref, ng_ref, nu_ref, nd_ref,
    big_sem, stage_sem, moment_sem, row_sem, own_sem, ssem, rsem, dssem, drsem, gssem, grsem,
):
    me = lax.axis_index("dp")
    right, left = lax.rem(me + 1, n), lax.rem(me + n - 1, n)
    towards = (right, left)
    tokens, dim = a_ref.shape
    hidden = wg_hbm.shape[2]
    layers = wg_hbm.shape[0]
    share, dshare = dim // n, hidden // n
    piece = dshare // 2
    owners = WIDE // piece
    blocks = hidden // WIDE
    halves = blocks // 2
    tiles = tokens // TILE

    def remote(src, dst, send, recv, to):
        return pltpu.make_async_remote_copy(src_ref=src, dst_ref=dst, send_sem=send, recv_sem=recv, device_id={"dp": to}, device_id_type=MESH)

    barrier = pltpu.get_barrier_semaphore()
    for to in towards:
        pl.semaphore_signal(barrier, inc=1, device_id={"dp": to}, device_id_type=MESH)

    loads = [pltpu.make_async_copy(s, t, big_sem.at[i]) for i, (s, t) in enumerate(((a1_hbm, a_ref), (dy_hbm, d_ref), (a1t_hbm, at_ref), (dyt_hbm, dt_ref)))]

    def unit_start(block, e):
        return ((lax.rem(block, halves) * owners + e) * 2 + block // halves) * piece

    def stage(number):
        layer, block, slot = layers - 1 - number // blocks, lax.rem(number, blocks), lax.rem(number, 2)
        copies = []
        for e in range(owners):
            at = pl.multiple_of(unit_start(block, e), piece)
            here = pl.ds(e * piece, piece)
            copies.append(pltpu.make_async_copy(wg_hbm.at[layer, :, pl.ds(at, piece)], sg_ref.at[slot, :, here], stage_sem.at[slot, 0, e]))
            copies.append(pltpu.make_async_copy(wu_hbm.at[layer, :, pl.ds(at, piece)], su_ref.at[slot, :, here], stage_sem.at[slot, 1, e]))
            copies.append(pltpu.make_async_copy(wd_hbm.at[layer, pl.ds(at, piece), :], sd_ref.at[slot, here, :], stage_sem.at[slot, 2, e]))
        return copies

    for copy in stage(jnp.int32(0)):
        copy.start()
    for copy in loads:
        copy.start()
    moments = [
        pltpu.make_async_copy(s, t, moment_sem.at[i])
        for i, (s, t) in enumerate(((mg_hbm, mg_ref), (mu_hbm, mu_ref), (md_hbm, md_ref), (vg_hbm, vg_ref), (vu_hbm, vu_ref), (vd_hbm, vd_ref)))
    ]
    rows = [
        pltpu.make_async_copy(wg_hbm.at[:, pl.ds(pl.multiple_of(me * share, share), share), :], ng_ref, row_sem.at[0]),
        pltpu.make_async_copy(wu_hbm.at[:, pl.ds(pl.multiple_of(me * share, share), share), :], nu_ref, row_sem.at[1]),
        pltpu.make_async_copy(wd_hbm.at[:, pl.ds(pl.multiple_of(me * dshare, dshare), dshare), :], nd_ref, row_sem.at[2]),
    ]
    for copy in moments + rows:
        copy.start()

    def whose(c, k):
        return lax.rem(me + n - 1 - k + n, n) if c == 0 else lax.rem(me + 1 + k, n)

    def ring(k, term, slot, send, recv, finish):
        for c in range(2):
            to = towards[c]

            @pl.when(k == 0)
            def _():
                remote(term(c, whose(c, 0)), slot(c, 0), send(c), recv(c, 0), to).start()

            @pl.when(k > 0)
            def _():
                came = slot(c, k - 1)
                copy = remote(came, came, send(c), recv(c, k - 1), to)
                copy.wait_recv()
                copy.wait_send()
                total = (came[...].astype(F32) + term(c, whose(c, k))[...].astype(F32)).astype(BF)

                @pl.when(k < n - 1)
                def _():
                    came[...] = total
                    remote(came, slot(c, k), send(c), recv(c, k), to).start()

                @pl.when(k == n - 1)
                def _():
                    finish(c, total)

    def wide_ring(number, k):
        layer, block, slot = layers - 1 - number // blocks, lax.rem(number, blocks), lax.rem(number, 2)

        def finish(c, total):
            out = (gg_out, gu_out)[c]
            for e in range(owners):
                out[layer, :, pl.ds(pl.multiple_of(unit_start(block, e), piece), piece)] = total[:, e * piece : (e + 1) * piece]

        ring(
            k,
            lambda c, who: (tg_ref, tu_ref)[c].at[slot, pl.ds(pl.multiple_of(who * share, share), share), :],
            lambda c, hop: (rg_ref, ru_ref)[c].at[slot, hop],
            lambda c: ssem.at[c],
            lambda c, hop: rsem.at[c, slot, hop],
            finish,
        )

    def down_ring(number, k):
        layer, half = layers - 1 - number // 2, lax.rem(number, 2)
        part = piece // 2

        def finish(c, total):
            gd_out[layer, pl.ds(pl.multiple_of(half * piece + c * part, part), part), :] = total

        ring(
            k,
            lambda c, who: td_ref.at[half, pl.ds(pl.multiple_of(who * piece + c * part, part), part), :],
            lambda c, hop: (rc_ref, rw_ref)[c].at[half, hop],
            lambda c: dssem.at[c],
            lambda c, hop: drsem.at[c, half, hop],
            finish,
        )

    def update(layer):
        for g_ref, m_ref, v_ref, w_ref in ((gg_out, mg_ref, vg_ref, ng_ref), (gu_out, mu_ref, vu_ref, nu_ref), (gd_out, md_ref, vd_ref, nd_ref)):
            new, _, _ = adamw(w_ref[layer].astype(F32), m_ref[layer], v_ref[layer], g_ref[layer].astype(F32))
            w_ref[layer] = new

    def own(layer):
        return [
            pltpu.make_async_copy(ng_ref.at[layer], og_ref.at[layer, pl.ds(pl.multiple_of(me * share, share), share), :], own_sem.at[layer, 0]),
            pltpu.make_async_copy(nu_ref.at[layer], ou_ref.at[layer, pl.ds(pl.multiple_of(me * share, share), share), :], own_sem.at[layer, 1]),
            pltpu.make_async_copy(nd_ref.at[layer], od_ref.at[layer, pl.ds(pl.multiple_of(me * dshare, dshare), dshare), :], own_sem.at[layer, 2]),
        ]

    def gather(layer, k):
        for u in range(3):
            for c in range(2):
                part = share // 2 if u < 2 else dshare // 2
                if u < 2:
                    mine = (ng_ref, nu_ref)[c].at[layer, pl.ds(u * part, part), :]
                    place = lambda who: (og_ref, ou_ref)[c].at[layer, pl.ds(pl.multiple_of(who * share + u * part, part), part), :]
                else:
                    mine = nd_ref.at[layer, pl.ds(c * part, part), :]
                    place = lambda who: od_ref.at[layer, pl.ds(pl.multiple_of(who * dshare + c * part, part), part), :]
                at = lax.rem(me + n - k, n) if c == 0 else lax.rem(me + k, n)
                send, recv, to = gssem.at[c, u], grsem.at[layer, c, u], towards[c]

                @pl.when(k == 0)
                def _():
                    remote(mine, place(me), send, recv.at[0], to).start()

                @pl.when(k > 0)
                def _():
                    copy = remote(mine, place(at), send, recv.at[k - 1], to)
                    copy.wait_recv()
                    copy.wait_send()

                    @pl.when(k < n - 1)
                    def _():
                        remote(place(at), place(at), send, recv.at[k], to).start()

    def block(number, needs_da, tick):
        slot = lax.rem(number, 2)
        for copy in stage(number):
            copy.wait()

        @pl.when(number + 1 < layers * blocks)
        def _():
            for copy in stage(number + 1):
                copy.start()

        base = pl.multiple_of(lax.rem(lax.rem(number, blocks), halves) * owners * piece, WIDE)
        half = lax.rem(number, blocks) // halves
        for s in range(WIDE // NARROW):
            cols = slice(s * NARROW, (s + 1) * NARROW)

            def tile(t):
                here = pl.ds(pl.multiple_of(t * TILE, TILE), TILE)
                wg, wu, wd = sg_ref[slot, :, cols], su_ref[slot, :, cols], sd_ref[slot, cols, :]
                a, d = a_ref[here, :], d_ref[here, :]
                g, u = dot(a, wg), dot(a, wu)
                dact = dot_nt(d, wd).astype(BF).astype(F32)
                sig = sigmoid(g)
                silu = g * sig
                act_ref[here, :] = (silu * u).astype(BF)
                du = (dact * silu).astype(BF)
                dg = (dact * u * (sig + silu * (1.0 - sig))).astype(BF)
                du_ref[here, :] = du
                dg_ref[here, :] = dg
                if needs_da:
                    da_ref[here, :] += dot_nt(dg, wg) + dot_nt(du, wu)

            def two(i, carry):
                tile(2 * i)
                tile(2 * i + 1)
                tick(s * (tiles // 2) + i)
                return carry

            lax.fori_loop(0, tiles // 2, two, 0)
            if s == 0:

                @pl.when(number == 0)
                def _():
                    loads[2].wait()
                    loads[3].wait()

            tg_ref[slot, :, cols] = dot(at_ref[...], dg_ref[...]).astype(BF)
            tu_ref[slot, :, cols] = dot(at_ref[...], du_ref[...]).astype(BF)
            td_ref[half, pl.ds(base + s * NARROW, NARROW), :] = dot(dt_ref[...], act_ref[...]).T.astype(BF)

    def tick(number, point):
        @pl.when(number > 0)
        def _():
            wide_ring(number - 1, point)

        @pl.when(jnp.logical_and(number > 1, lax.rem(point, 2) == 1))
        def _():
            down_ring(number // 2 - 1, lax.rem(number, 2) * (n // 2) + point // 2)

    loads[0].wait()
    loads[1].wait()
    da_ref[...] = jnp.zeros_like(da_ref)
    pl.semaphore_wait(barrier, 2)

    def last_layer(number, carry):
        block(number, True, lambda point: tick(number, point))
        return carry

    lax.fori_loop(0, blocks, last_layer, 0)

    h_load = pltpu.make_async_copy(h_hbm, a_ref, big_sem.at[0])
    h_load.start()
    at_load = pltpu.make_async_copy(a0t_hbm, at_ref, big_sem.at[2])
    at_load.start()
    h_load.wait()

    def through_norm(t, carry):
        here = pl.ds(pl.multiple_of(t * TILE, TILE), TILE)
        h = a_ref[here, :].astype(F32)
        scale = norm_scale(h)
        da = da_ref[here, :].astype(BF).astype(F32)
        mean = jnp.mean(da * h, -1, keepdims=True)
        back = (scale * (da - h * (scale * scale * mean))).astype(BF).astype(F32)
        dh = (d_ref[here, :].astype(F32) + back).astype(BF)
        d_ref[here, :] = dh
        dt_ref[:, here] = dh.T
        return carry

    lax.fori_loop(0, tiles, through_norm, 0)
    a_load = pltpu.make_async_copy(a0_hbm, a_ref, big_sem.at[1])
    a_load.start()
    a_load.wait()
    at_load.wait()

    def first_layer(number, carry):
        block(number, False, lambda point: tick(number, point))
        return carry

    lax.fori_loop(blocks, blocks + halves, first_layer, 0)
    for copy in moments + rows:
        copy.wait()
    update(layers - 1)
    for copy in own(layers - 1):
        copy.start()
    lax.fori_loop(blocks + halves, 2 * blocks, first_layer, 0)

    def end(k, carry):
        wide_ring(2 * blocks - 1, k)
        down_ring(3, k)
        gather(layers - 1, k)
        return carry

    lax.fori_loop(0, n, end, 0)
    update(0)
    for copy in own(0):
        copy.start()

    def gather0(k, carry):
        gather(0, k)
        return carry

    lax.fori_loop(0, n, gather0, 0)
    for layer in range(layers):
        for copy in own(layer):
            copy.wait()


def rest(n, states, dy, w, m, v):
    tokens, dim = dy.shape
    layers, _, hidden = w[0].shape
    share, dshare = dim // n, hidden // n
    sds = jax.ShapeDtypeStruct
    dma = pltpu.SemaphoreType.DMA
    hops = n - 1
    return pl.pallas_call(
        functools.partial(rest_kernel, n),
        in_specs=[ANY] * 16,
        out_specs=[ANY] * 3 + [VMEM] * 3,
        out_shape=[sds(t.shape, BF) for t in w] + [sds(t.shape, BF) for t in m],
        scratch_shapes=[
            pltpu.VMEM((tokens, dim), BF),
            pltpu.VMEM((dim, tokens), BF),
            pltpu.VMEM((tokens, dim), BF),
            pltpu.VMEM((dim, tokens), BF),
            pltpu.VMEM((tokens, dim), F32),
            pltpu.VMEM((tokens, NARROW), BF),
            pltpu.VMEM((tokens, NARROW), BF),
            pltpu.VMEM((tokens, NARROW), BF),
            pltpu.VMEM((2, dim, WIDE), BF),
            pltpu.VMEM((2, dim, WIDE), BF),
            pltpu.VMEM((2, WIDE, dim), BF),
            pltpu.VMEM((2, dim, WIDE), BF),
            pltpu.VMEM((2, dim, WIDE), BF),
            pltpu.VMEM((2, hidden // 2, dim), BF),
            pltpu.VMEM((2, hops, share, WIDE), BF),
            pltpu.VMEM((2, hops, share, WIDE), BF),
            pltpu.VMEM((2, hops, dshare // 4, dim), BF),
            pltpu.VMEM((2, hops, dshare // 4, dim), BF),
            *[pltpu.VMEM(t.shape, F32) for t in (*m, *v)],
            *[pltpu.VMEM(t.shape, BF) for t in m],
            dma((4,)),
            dma((2, 3, WIDE // (dshare // 2))),
            dma((6,)),
            dma((3,)),
            dma((layers, 3)),
            dma((2,)),
            dma((2, 2, hops)),
            dma((2,)),
            dma((2, 2, hops)),
            dma((2, 3)),
            dma((layers, 2, 3, hops)),
        ],
        compiler_params=pltpu.CompilerParams(vmem_limit_bytes=VMEM_LIMIT, collective_id=0, has_side_effects=True),
        name="rest",
    )(*states, dy, *w, *m, *v)


def solution(mesh):
    n = mesh.shape["dp"]

    def step(x, dy, *arrays):
        w, m, v = (arrays[i : i + 3] for i in (0, 3, 6))
        x, dy = x[0], dy[0]
        states = forward(x, dy, *w)
        *new, gg, gu, gd = rest(n, states, dy, w, m, v)
        moments = [adamw(jnp.zeros((), F32), m, v, g.astype(F32))[1:] for m, v, g in zip(m, v, (gg, gu, gd), strict=True)]
        return (*new, *(one[0] for one in moments), *(one[1] for one in moments))

    seq, whole, block = P(("rep", "dp"), None, None), P(None, None, None), P(None, "dp", None)
    return jax.shard_map(
        step,
        mesh=mesh,
        in_specs=(seq, seq, *[whole] * 3, *[block] * 6),
        out_specs=(*[P("rep", None, None)] * 3, *[P("rep", "dp", None)] * 6),
        check_vma=False,
    )
```

```python
import functools

import jax
import jax.numpy as jnp
from jax import lax
from jax.experimental import pallas as pl
from jax.experimental.pallas import tpu as pltpu
from jax.sharding import PartitionSpec as P

F32, BF = jnp.float32, jnp.bfloat16
NT = (((1,), (1,)), ((), ()))
MESH = pl.DeviceIdType.MESH
VMEM_LIMIT = 66_000_000
WIDE = 512
NARROW = 256
TILE = 512
SLOTS = 4
ANY = pl.BlockSpec(memory_space=pl.ANY)
VMEM = pl.BlockSpec(memory_space=pltpu.VMEM)


def dot(a, b):
    return jnp.dot(a, b, preferred_element_type=F32)


def dot_nt(a, b):
    return lax.dot_general(a, b, NT, preferred_element_type=F32)


def sigmoid(g):
    return 0.5 * jnp.tanh(0.5 * g) + 0.5


def norm_scale(wide):
    return lax.rsqrt(jnp.mean(wide * wide, -1, keepdims=True) + 1e-6)


def adamw(w, m, v, g):
    m = 0.9 * m + 0.1 * g
    v = 0.95 * v + 0.05 * g * g
    step = m * lax.rsqrt(v + 1e-8) + 0.1 * w
    return (w - 0.02 * step).astype(BF), m, v


def forward_kernel(x_ref, dy_ref, wg_ref, wu_ref, wd_ref, h_ref, a0_ref, a1_ref, a0t_ref, a1t_ref, dyt_ref):
    x = x_ref[...].astype(F32)
    a = (x * norm_scale(x)).astype(BF)
    a0_ref[...] = a
    a0t_ref[...] = a.T
    dyt_ref[...] = dy_ref[...].T
    acc = None
    for at in range(0, wg_ref.shape[1], WIDE):
        cols = slice(at, at + WIDE)
        g = dot(a, wg_ref[:, cols])
        u = dot(a, wu_ref[:, cols])
        part = dot((g * sigmoid(g) * u).astype(BF), wd_ref[cols, :])
        acc = part if acc is None else acc + part
    h = (x + acc.astype(BF).astype(F32)).astype(BF)
    h_ref[...] = h
    wide = h.astype(F32)
    a1 = (wide * norm_scale(wide)).astype(BF)
    a1_ref[...] = a1
    a1t_ref[...] = a1.T


def forward(x, dy, wg, wu, wd):
    tokens, dim = x.shape
    row = pl.BlockSpec((TILE, dim), lambda i: (i, 0))
    col = pl.BlockSpec((dim, TILE), lambda i: (0, i))
    first = lambda w: pl.BlockSpec((None, *w.shape[1:]), lambda i: (0, 0, 0))
    return pl.pallas_call(
        forward_kernel,
        grid=(tokens // TILE,),
        in_specs=[row, row, first(wg), first(wu), first(wd)],
        out_specs=[row] * 3 + [col] * 3,
        out_shape=[jax.ShapeDtypeStruct((tokens, dim), BF)] * 3 + [jax.ShapeDtypeStruct((dim, tokens), BF)] * 3,
        compiler_params=pltpu.CompilerParams(vmem_limit_bytes=VMEM_LIMIT),
        name="forward0",
    )(x, dy, wg, wu, wd)


def rest_kernel(
    n, h_hbm, a0_hbm, a1_hbm, a0t_hbm, a1t_hbm, dyt_hbm, dy_hbm, wg_hbm, wu_hbm, wd_hbm, mg_hbm, mu_hbm, md_hbm, vg_hbm, vu_hbm, vd_hbm,
    og_ref, ou_ref, od_ref, gg_out, gu_out, gd_out,
    a_ref, at_ref, d_ref, dt_ref, da_ref, act_ref, dg_ref, du_ref, sg_ref, su_ref, sd_ref, tg_ref, tu_ref, td_ref,
    rg_ref, ru_ref, rc_ref, rw_ref, mg_ref, mu_ref, md_ref, vg_ref, vu_ref, vd_ref, ng_ref, nu_ref, nd_ref,
    big_sem, stage_sem, moment_sem, row_sem, own_sem, ssem, rsem, dssem, drsem, gssem, grsem,
):
    me = lax.axis_index("dp")
    right, left = lax.rem(me + 1, n), lax.rem(me + n - 1, n)
    towards = (right, left)
    tokens, dim = a_ref.shape
    hidden = wg_hbm.shape[2]
    layers = wg_hbm.shape[0]
    share, dshare = dim // n, hidden // n
    piece = dshare // 2
    owners = WIDE // piece
    blocks = hidden // WIDE
    halves = blocks // 2
    tiles = tokens // TILE

    def remote(src, dst, send, recv, to):
        return pltpu.make_async_remote_copy(src_ref=src, dst_ref=dst, send_sem=send, recv_sem=recv, device_id={"dp": to}, device_id_type=MESH)

    barrier = pltpu.get_barrier_semaphore()
    for to in towards:
        pl.semaphore_signal(barrier, inc=1, device_id={"dp": to}, device_id_type=MESH)

    loads = [pltpu.make_async_copy(s, t, big_sem.at[i]) for i, (s, t) in enumerate(((a1_hbm, a_ref), (dy_hbm, d_ref), (a1t_hbm, at_ref), (dyt_hbm, dt_ref)))]

    def unit_start(block, e):
        return ((lax.rem(block, halves) * owners + e) * 2 + block // halves) * piece

    def stage(number):
        layer, block, slot = layers - 1 - number // blocks, lax.rem(number, blocks), lax.rem(number, 2)
        copies = []
        for e in range(owners):
            at = pl.multiple_of(unit_start(block, e), piece)
            here = pl.ds(e * piece, piece)
            copies.append(pltpu.make_async_copy(wg_hbm.at[layer, :, pl.ds(at, piece)], sg_ref.at[slot, :, here], stage_sem.at[slot, 0, e]))
            copies.append(pltpu.make_async_copy(wu_hbm.at[layer, :, pl.ds(at, piece)], su_ref.at[slot, :, here], stage_sem.at[slot, 1, e]))
            copies.append(pltpu.make_async_copy(wd_hbm.at[layer, pl.ds(at, piece), :], sd_ref.at[slot, here, :], stage_sem.at[slot, 2, e]))
        return copies

    for copy in stage(jnp.int32(0)):
        copy.start()
    for copy in loads:
        copy.start()
    moments = [
        pltpu.make_async_copy(s, t, moment_sem.at[i])
        for i, (s, t) in enumerate(((mg_hbm, mg_ref), (mu_hbm, mu_ref), (md_hbm, md_ref), (vg_hbm, vg_ref), (vu_hbm, vu_ref), (vd_hbm, vd_ref)))
    ]
    rows = [
        pltpu.make_async_copy(wg_hbm.at[:, pl.ds(pl.multiple_of(me * share, share), share), :], ng_ref, row_sem.at[0]),
        pltpu.make_async_copy(wu_hbm.at[:, pl.ds(pl.multiple_of(me * share, share), share), :], nu_ref, row_sem.at[1]),
        pltpu.make_async_copy(wd_hbm.at[:, pl.ds(pl.multiple_of(me * dshare, dshare), dshare), :], nd_ref, row_sem.at[2]),
    ]
    for copy in moments + rows:
        copy.start()

    def whose(c, k):
        return lax.rem(me + n - 1 - k + n, n) if c == 0 else lax.rem(me + 1 + k, n)

    def ring(k, term, slot, send, recv, finish):
        k = jnp.asarray(k, jnp.int32)
        for c in range(2):
            to = towards[c]

            @pl.when(k == 0)
            def _():
                remote(term(c, whose(c, 0)), slot(c, 0), send(c), recv(c, 0), to).start()

            @pl.when(k > 0)
            def _():
                came = slot(c, k - 1)
                copy = remote(came, came, send(c), recv(c, k - 1), to)
                copy.wait_recv()
                copy.wait_send()
                total = (came[...].astype(F32) + term(c, whose(c, k))[...].astype(F32)).astype(BF)

                @pl.when(k < n - 1)
                def _():
                    came[...] = total
                    remote(came, slot(c, k), send(c), recv(c, k), to).start()

                @pl.when(k == n - 1)
                def _():
                    finish(c, total)

    def wide_ring(number, k):
        layer, block, slot = layers - 1 - number // blocks, lax.rem(number, blocks), lax.rem(number, SLOTS)

        def finish(c, total):
            out = (gg_out, gu_out)[c]
            for e in range(owners):
                out[layer, :, pl.ds(pl.multiple_of(unit_start(block, e), piece), piece)] = total[:, e * piece : (e + 1) * piece]

        ring(
            k,
            lambda c, who: (tg_ref, tu_ref)[c].at[slot, pl.ds(pl.multiple_of(who * share, share), share), :],
            lambda c, hop: (rg_ref, ru_ref)[c].at[slot, hop],
            lambda c: ssem.at[c, slot],
            lambda c, hop: rsem.at[c, slot, hop],
            finish,
        )

    def down_ring(number, k):
        layer, half = layers - 1 - number // 2, lax.rem(number, 2)
        part = piece // 2

        def finish(c, total):
            gd_out[layer, pl.ds(pl.multiple_of(half * piece + c * part, part), part), :] = total

        ring(
            k,
            lambda c, who: td_ref.at[half, pl.ds(pl.multiple_of(who * piece + c * part, part), part), :],
            lambda c, hop: (rc_ref, rw_ref)[c].at[half, hop],
            lambda c: dssem.at[c],
            lambda c, hop: drsem.at[c, half, hop],
            finish,
        )

    def update(layer):
        for g_ref, m_ref, v_ref, w_ref in ((gg_out, mg_ref, vg_ref, ng_ref), (gu_out, mu_ref, vu_ref, nu_ref), (gd_out, md_ref, vd_ref, nd_ref)):
            new, _, _ = adamw(w_ref[layer].astype(F32), m_ref[layer], v_ref[layer], g_ref[layer].astype(F32))
            w_ref[layer] = new

    def own(layer):
        return [
            pltpu.make_async_copy(ng_ref.at[layer], og_ref.at[layer, pl.ds(pl.multiple_of(me * share, share), share), :], own_sem.at[layer, 0]),
            pltpu.make_async_copy(nu_ref.at[layer], ou_ref.at[layer, pl.ds(pl.multiple_of(me * share, share), share), :], own_sem.at[layer, 1]),
            pltpu.make_async_copy(nd_ref.at[layer], od_ref.at[layer, pl.ds(pl.multiple_of(me * dshare, dshare), dshare), :], own_sem.at[layer, 2]),
        ]

    def gather(layer, k):
        for u in range(3):
            for c in range(2):
                part = share // 2 if u < 2 else dshare // 2
                if u < 2:
                    mine = (ng_ref, nu_ref)[c].at[layer, pl.ds(u * part, part), :]
                    place = lambda who: (og_ref, ou_ref)[c].at[layer, pl.ds(pl.multiple_of(who * share + u * part, part), part), :]
                else:
                    mine = nd_ref.at[layer, pl.ds(c * part, part), :]
                    place = lambda who: od_ref.at[layer, pl.ds(pl.multiple_of(who * dshare + c * part, part), part), :]
                at = lax.rem(me + n - k, n) if c == 0 else lax.rem(me + k, n)
                send, recv, to = gssem.at[c, u], grsem.at[layer, c, u], towards[c]

                @pl.when(k == 0)
                def _():
                    remote(mine, place(me), send, recv.at[0], to).start()

                @pl.when(k > 0)
                def _():
                    copy = remote(mine, place(at), send, recv.at[k - 1], to)
                    copy.wait_recv()
                    copy.wait_send()

                    @pl.when(k < n - 1)
                    def _():
                        remote(place(at), place(at), send, recv.at[k], to).start()

    def block(number, needs_da, tick):
        slot, kept = lax.rem(number, 2), lax.rem(number, SLOTS)
        for copy in stage(number):
            copy.wait()

        @pl.when(number + 1 < layers * blocks)
        def _():
            for copy in stage(number + 1):
                copy.start()

        base = pl.multiple_of(lax.rem(lax.rem(number, blocks), halves) * owners * piece, WIDE)
        half = lax.rem(number, blocks) // halves
        def narrow(s, carry):
            cols = pl.ds(pl.multiple_of(s * NARROW, NARROW), NARROW)

            def tile(t):
                here = pl.ds(pl.multiple_of(t * TILE, TILE), TILE)
                wg, wu, wd = sg_ref[slot, :, cols], su_ref[slot, :, cols], sd_ref[slot, cols, :]
                a, d = a_ref[here, :], d_ref[here, :]
                g, u = dot(a, wg), dot(a, wu)
                dact = dot_nt(d, wd).astype(BF).astype(F32)
                sig = sigmoid(g)
                silu = g * sig
                act_ref[here, :] = (silu * u).astype(BF)
                du = (dact * silu).astype(BF)
                dg = (dact * u * (sig + silu * (1.0 - sig))).astype(BF)
                du_ref[here, :] = du
                dg_ref[here, :] = dg
                if needs_da:
                    da_ref[here, :] += dot_nt(dg, wg) + dot_nt(du, wu)

            def two(first, i, carry):
                tile(first + 2 * i)
                tile(first + 2 * i + 1)
                return carry

            def half_of_tiles(i, carry):
                lax.fori_loop(0, tiles // 4, functools.partial(two, i * (tiles // 2)), 0)

                @pl.when(i == 0)
                def _():
                    tick(True, 2 * s)

                @pl.when(i == 1)
                def _():
                    tick(False, 2 * s)

                return carry

            lax.fori_loop(0, 2, half_of_tiles, 0)

            @pl.when(jnp.logical_and(number == 0, s == 0))
            def _():
                loads[2].wait()
                loads[3].wait()

            tg_ref[kept, :, cols] = dot(at_ref[...], dg_ref[...]).astype(BF)
            tu_ref[kept, :, cols] = dot(at_ref[...], du_ref[...]).astype(BF)
            tick(True, 2 * s + 1)
            td_ref[half, pl.ds(pl.multiple_of(base + s * NARROW, NARROW), NARROW), :] = dot(dt_ref[...], act_ref[...]).T.astype(BF)
            tick(False, 2 * s + 1)
            return carry

        lax.fori_loop(0, WIDE // NARROW, narrow, 0)

    def tick(number, wide, turn):
        if wide:

            @pl.when(number > 1)
            def _():
                wide_ring(number - 2, n // 2 + turn)

            @pl.when(number > 0)
            def _():
                wide_ring(number - 1, turn)

        else:

            @pl.when(number > 1)
            def _():
                down_ring(number // 2 - 1, lax.rem(number, 2) * (n // 2) + turn)

    loads[0].wait()
    loads[1].wait()
    da_ref[...] = jnp.zeros_like(da_ref)
    pl.semaphore_wait(barrier, 2)

    def last_layer(number, carry):
        block(number, True, functools.partial(tick, number))
        return carry

    lax.fori_loop(0, blocks, last_layer, 0)

    h_load = pltpu.make_async_copy(h_hbm, a_ref, big_sem.at[0])
    h_load.start()
    at_load = pltpu.make_async_copy(a0t_hbm, at_ref, big_sem.at[2])
    at_load.start()
    h_load.wait()

    def through_norm(t, carry):
        here = pl.ds(pl.multiple_of(t * TILE, TILE), TILE)
        h = a_ref[here, :].astype(F32)
        scale = norm_scale(h)
        da = da_ref[here, :].astype(BF).astype(F32)
        mean = jnp.mean(da * h, -1, keepdims=True)
        back = (scale * (da - h * (scale * scale * mean))).astype(BF).astype(F32)
        dh = (d_ref[here, :].astype(F32) + back).astype(BF)
        d_ref[here, :] = dh
        dt_ref[:, here] = dh.T
        return carry

    lax.fori_loop(0, tiles, through_norm, 0)
    a_load = pltpu.make_async_copy(a0_hbm, a_ref, big_sem.at[1])
    a_load.start()
    a_load.wait()
    at_load.wait()

    def first_layer(number, carry):
        block(number, False, functools.partial(tick, number))
        return carry

    lax.fori_loop(blocks, blocks + halves, first_layer, 0)
    for copy in moments + rows:
        copy.wait()
    update(layers - 1)
    for copy in own(layers - 1):
        copy.start()
    lax.fori_loop(blocks + halves, 2 * blocks, first_layer, 0)

    def end(k, carry):
        @pl.when(k < n // 2)
        def _():
            wide_ring(layers * blocks - 2, n // 2 + k)

        wide_ring(layers * blocks - 1, k)
        down_ring(2 * layers - 1, k)
        gather(layers - 1, k)
        return carry

    lax.fori_loop(0, n, end, 0)
    update(0)
    for copy in own(0):
        copy.start()

    def gather0(k, carry):
        gather(0, k)
        return carry

    lax.fori_loop(0, n, gather0, 0)
    for layer in range(layers):
        for copy in own(layer):
            copy.wait()


def rest(n, states, dy, w, m, v):
    tokens, dim = dy.shape
    layers, _, hidden = w[0].shape
    share, dshare = dim // n, hidden // n
    sds = jax.ShapeDtypeStruct
    dma = pltpu.SemaphoreType.DMA
    hops = n - 1
    return pl.pallas_call(
        functools.partial(rest_kernel, n),
        in_specs=[ANY] * 16,
        out_specs=[ANY] * 3 + [VMEM] * 3,
        out_shape=[sds(t.shape, BF) for t in w] + [sds(t.shape, BF) for t in m],
        scratch_shapes=[
            pltpu.VMEM((tokens, dim), BF),
            pltpu.VMEM((dim, tokens), BF),
            pltpu.VMEM((tokens, dim), BF),
            pltpu.VMEM((dim, tokens), BF),
            pltpu.VMEM((tokens, dim), F32),
            pltpu.VMEM((tokens, NARROW), BF),
            pltpu.VMEM((tokens, NARROW), BF),
            pltpu.VMEM((tokens, NARROW), BF),
            pltpu.VMEM((2, dim, WIDE), BF),
            pltpu.VMEM((2, dim, WIDE), BF),
            pltpu.VMEM((2, WIDE, dim), BF),
            pltpu.VMEM((SLOTS, dim, WIDE), BF),
            pltpu.VMEM((SLOTS, dim, WIDE), BF),
            pltpu.VMEM((2, hidden // 2, dim), BF),
            pltpu.VMEM((SLOTS, hops, share, WIDE), BF),
            pltpu.VMEM((SLOTS, hops, share, WIDE), BF),
            pltpu.VMEM((2, hops, dshare // 4, dim), BF),
            pltpu.VMEM((2, hops, dshare // 4, dim), BF),
            *[pltpu.VMEM(t.shape, F32) for t in (*m, *v)],
            *[pltpu.VMEM(t.shape, BF) for t in m],
            dma((4,)),
            dma((2, 3, WIDE // (dshare // 2))),
            dma((6,)),
            dma((3,)),
            dma((layers, 3)),
            dma((2, SLOTS)),
            dma((2, SLOTS, hops)),
            dma((2,)),
            dma((2, 2, hops)),
            dma((2, 3)),
            dma((layers, 2, 3, hops)),
        ],
        compiler_params=pltpu.CompilerParams(vmem_limit_bytes=VMEM_LIMIT, collective_id=0, has_side_effects=True),
        name="rest",
    )(*states, dy, *w, *m, *v)


def solution(mesh):
    n = mesh.shape["dp"]

    def step(x, dy, *arrays):
        w, m, v = (arrays[i : i + 3] for i in (0, 3, 6))
        x, dy = x[0], dy[0]
        states = forward(x, dy, *w)
        *new, gg, gu, gd = rest(n, states, dy, w, m, v)
        moments = [adamw(jnp.zeros((), F32), m, v, g.astype(F32))[1:] for m, v, g in zip(m, v, (gg, gu, gd), strict=True)]
        return (*new, *(one[0] for one in moments), *(one[1] for one in moments))

    seq, whole, block = P(("rep", "dp"), None, None), P(None, None, None), P(None, "dp", None)
    return jax.shard_map(
        step,
        mesh=mesh,
        in_specs=(seq, seq, *[whole] * 3, *[block] * 6),
        out_specs=(*[P("rep", None, None)] * 3, *[P("rep", "dp", None)] * 6),
        check_vma=False,
    )
```
